32 devices in a mesh: grid: 8 (over z, x), orb: 4 (over y, core).
Axes of the slice: x: 2, y: 2, z: 4, core: 2. Of those that a mesh axis runs over, the one named last changes fastest.
Arguments:
- orbitals: bfloat16 [1800, 65536], P('orb', 'grid'), may hold values from -0.5 to 1.5
- pivots: int32 [3, 96], replicated, may hold values from 0 to 65535, as said below
Outputs:
- cholesky_factor: float32 [65536, 288], P(('grid', 'orb'))
- residual_diagonal: float32 [65536], P(('grid', 'orb'))
- diagonal_peaks: float32 [3], replicated
The draws below stay inside these ranges and needn't reach their ends.
Inputs may be any that keep to these rules, and one draw needn't show every extreme that they name: `pivots`: all 3 x 96 pivot indices are distinct grid points.
All inputs are finite; a program needn't handle non-finite values.
Results may differ from the reference program's by a relative error of at most 0.0003.
Values may be sent and summed in bfloat16 or wider, within the bound.
A program may use at most 64 MiB of HBM per device.

```python
import jax
import jax.numpy as jnp
from jax import lax

ORB = 1800
PIV = 96
STEPS = 3
GRID_POINTS = 65536


def draw_pivots(key, part):
    order = jax.random.permutation(jax.random.fold_in(key, 11), GRID_POINTS)
    return order[:STEPS * PIV].reshape(STEPS, PIV).astype(jnp.int32)


def levels(stream_key, shape, pieces, smallest, largest):
    def one(axis_at, parts):
        draws = jax.random.uniform(jax.random.fold_in(jax.random.fold_in(stream_key, 6), axis_at), (parts,), jnp.float32, smallest / len(pieces), largest / len(pieces))
        return jnp.repeat(jnp.exp(draws), shape[axis_at] // parts).reshape((-1,) + (1,) * (len(shape) - axis_at - 1))

    loudness = one(*pieces[0])
    for cut in pieces[1:]:
        loudness = loudness * one(*cut)
    return loudness


def setup_inputs(seed: int = 0) -> dict:
    keys = jax.random.split(jax.random.key(seed), 3)
    orbitals = jnp.clip(-0.5 + 2.0 * jax.random.uniform(keys[0], (ORB, GRID_POINTS), jnp.float32) ** levels(keys[0], (ORB, GRID_POINTS), ((0, 4), (1, 8)), -0.2, 0.2), -0.5, 1.5).astype(jnp.bfloat16)
    pivots = draw_pivots(jax.random.fold_in(keys[2], 71), 0)
    return dict(orbitals=orbitals, pivots=pivots)


def reference(orbitals, pivots):
    grid_count = orbitals.shape[1]
    squares = jnp.sum(jnp.square(orbitals.astype(jnp.float32)), axis=0)
    diagonal = jnp.square(squares / ORB)
    factor = jnp.zeros((grid_count, STEPS * PIV), jnp.float32)
    peaks = []
    for section in range(STEPS):
        chosen = pivots[section]
        sampled = jnp.take(orbitals, chosen, axis=1)
        known = jnp.take(factor, chosen, axis=0)
        pair = lax.dot_general(sampled.astype(jnp.float32), sampled.astype(jnp.float32), (((0,), (0,)), ((), ())), preferred_element_type=jnp.float32)
        block = jnp.square(pair / ORB) - jnp.dot(known, known.T, precision=lax.Precision.HIGHEST)
        inner = lax.dot_general(orbitals.astype(jnp.float32), sampled.astype(jnp.float32), (((0,), (0,)), ((), ())), preferred_element_type=jnp.float32)
        columns = jnp.square(inner / ORB) - jnp.dot(factor, known.T, precision=lax.Precision.HIGHEST)
        lower = jnp.linalg.cholesky(block)
        fresh = jax.scipy.linalg.solve_triangular(lower, columns.T, lower=True).T
        factor = factor.at[:, section * PIV:(section + 1) * PIV].set(fresh)
        diagonal = diagonal - jnp.sum(fresh * fresh, axis=1)
        peaks.append(jnp.max(diagonal))
    return (factor, diagonal, jnp.stack(peaks))
```

```python
import functools

import jax
import jax.numpy as jnp
from jax import lax
from jax.experimental import pallas as pl
from jax.experimental.pallas import tpu as pltpu
from jax.sharding import PartitionSpec as P

F32 = jnp.float32
BF16 = jnp.bfloat16
HIGHEST = lax.Precision.HIGHEST
MESH = pl.DeviceIdType.MESH
BLOCK = 48
PARTS = 4


def dot_nn(a, b, precision=None):
    return lax.dot_general(
        a, b, (((1,), (0,)), ((), ())), precision=precision, preferred_element_type=F32
    )


def dot_nt(a, b, precision=None):
    return lax.dot_general(
        a, b, (((1,), (1,)), ((), ())), precision=precision, preferred_element_type=F32
    )


def dot_tn(a, b, precision=None):
    return lax.dot_general(
        a, b, (((0,), (0,)), ((), ())), precision=precision, preferred_element_type=F32
    )


def eliminate_small(t, size):
    row_at = lax.broadcasted_iota(jnp.int32, t.shape, 0)
    for k in range(size):
        scale = lax.rsqrt(t[k : k + 1, k : k + 1])
        row = t[k : k + 1, :] * scale
        column = t[:, k : k + 1] * scale
        t = jnp.where(row_at > k, t - column * row, jnp.where(row_at == k, row, t))
    return t


def kernel(
    n_grid, n_orb, steps, orbitals_count,
    orb_hbm, piv_ref,
    factor_hbm, diag_ref, peaks_ref,
    own, other, mine, total, heard, swap, sums, arrived, local, pair_send, pair_recv,
    aug, out_v, tile_mine, tile_orb, tile_grid,
    load_sem, out_sem, x_send, x_recv, p1_send, p1_recv, p2_send, p2_recv,
    c_send, c_recv, q_send, q_recv, h_send, h_recv, s_send, s_recv,
    mo_send, mo_recv, mg_send, mg_recv,
):
    g = lax.axis_index("grid")
    o = lax.axis_index("orb")
    core = lax.rem(o, 2)
    side = o // 2
    mate = o + 1 - 2 * core
    across = (1 - side) * 2 + core
    share = own.shape[2]
    slots, slot_rows, _ = mine.shape
    rank = slots * slot_rows
    part = share // PARTS
    rows = share * n_orb

    loads = []
    for b in range(n_orb):
        copy = pltpu.make_async_copy(
            orb_hbm.at[:, pl.ds(b * share, share)], own.at[b], load_sem.at[b]
        )
        copy.start()
        loads.append(copy)

    barrier = pltpu.get_barrier_semaphore()
    for d in range(1, n_grid):
        pl.semaphore_signal(
            barrier, inc=1, device_id=(lax.rem(g + d, n_grid), o), device_id_type=MESH
        )
    for d in range(1, n_orb):
        pl.semaphore_signal(
            barrier, inc=1, device_id=(g, lax.rem(o + d, n_orb)), device_id_type=MESH
        )
    pl.semaphore_wait(barrier, n_grid + n_orb - 2)

    crossing = []
    for yy in range(2):
        start = pl.multiple_of((yy * 2 + 1 - core) * share, share)
        copy = pltpu.make_async_remote_copy(
            src_ref=orb_hbm.at[:, pl.ds(start, share)],
            dst_ref=other.at[yy],
            send_sem=x_send.at[yy],
            recv_sem=x_recv.at[yy],
            device_id=(g, mate),
            device_id_type=MESH,
        )
        copy.start()
        crossing.append(copy)

    base = g * rows
    wanted = piv_ref[...] - base
    picked = None
    for b in range(n_orb):
        loads[b].wait()
        lanes = lax.broadcasted_iota(jnp.int32, (rank, share), 1) + b * share
        hot = jnp.where(lanes == wanted, 1.0, 0.0).astype(BF16)
        term = dot_nt(hot, own[b])
        picked = term if picked is None else picked + term
    picked = picked.astype(BF16)
    for s in range(slots):
        mine[s] = picked[s * slot_rows : (s + 1) * slot_rows]

    def first(d):
        target = lax.rem(g + d, n_grid)
        return target, pltpu.make_async_remote_copy(
            src_ref=mine.at[lax.rem(target, slots)],
            dst_ref=heard.at[d],
            send_sem=p1_send.at[d],
            recv_sem=p1_recv.at[d],
            device_id=(target, o),
            device_id_type=MESH,
        )

    def second(d):
        target = lax.rem(g + d, n_grid)
        return pltpu.make_async_remote_copy(
            src_ref=heard.at[0],
            dst_ref=total.at[lax.rem(g, slots)],
            send_sem=p2_send.at[d],
            recv_sem=p2_recv.at[d],
            device_id=(target, o),
            device_id_type=MESH,
        )

    for d in range(1, n_grid):
        target, copy = first(d)

        @pl.when(target < slots)
        def _(copy=copy):
            copy.start()

    @pl.when(g < slots)
    def _():
        added = mine[lax.rem(g, slots)]
        for d in range(1, n_grid):
            first(d)[1].wait_recv()
            added = added + heard[d]
        heard[0] = added
        for d in range(1, n_grid):
            second(d).start()
        total[lax.rem(g, slots)] = added

    for d in range(1, n_grid):
        source = lax.rem(g + n_grid - d, n_grid)

        @pl.when(source < slots)
        def _(d=d):
            second(d).wait_recv()

    swap_copy = pltpu.make_async_remote_copy(
        src_ref=total, dst_ref=swap, send_sem=c_send, recv_sem=c_recv,
        device_id=(g, mate), device_id_type=MESH,
    )
    swap_copy.start()
    here = jnp.reshape(total[...], (rank, total.shape[2]))
    pair_here = dot_nt(here, here)
    swap_copy.wait_recv()
    there = jnp.reshape(swap[...], (rank, swap.shape[2]))
    pair = pair_here + dot_nt(there, there)
    half = rank // 2
    for h in range(2):
        pair_send[h] = pair[h * half : (h + 1) * half]
    pair_copy = pltpu.make_async_remote_copy(
        src_ref=pair_send.at[core], dst_ref=pair_recv.at[0], send_sem=q_send, recv_sem=q_recv,
        device_id=(g, across), device_id_type=MESH,
    )
    pair_copy.start()

    for copy in crossing:
        copy.wait_recv()

    def products(block, yy, p):
        lo = p * part
        a = own[block, :, lo : lo + part]
        b = other[yy, :, lo : lo + part]
        inner = dot_nn(here, a) + dot_nn(there, b)
        a32 = a.astype(F32)
        b32 = b.astype(F32)
        squares = jnp.sum(a32 * a32, axis=0, keepdims=True) + jnp.sum(
            b32 * b32, axis=0, keepdims=True
        )
        return inner, squares

    travel = []
    for p in range(PARTS):
        inner, squares = products(across, 1 - side, p)
        sums[p, 0:rank, :] = inner
        sums[p, rank : rank + 8, :] = jnp.broadcast_to(squares, (8, part))
        copy = pltpu.make_async_remote_copy(
            src_ref=sums.at[p], dst_ref=arrived.at[p],
            send_sem=s_send.at[p], recv_sem=s_recv.at[p],
            device_id=(g, across), device_id_type=MESH,
        )
        copy.start()
        travel.append(copy)

    pair_copy.wait_recv()
    half_copy = pltpu.make_async_remote_copy(
        src_ref=pair_recv.at[0], dst_ref=pair_recv.at[1], send_sem=h_send, recv_sem=h_recv,
        device_id=(g, mate), device_id_type=MESH,
    )
    half_copy.start()
    for p in range(PARTS):
        inner, squares = products(o, side, p)
        local[p, 0:rank, :] = inner
        local[p, rank : rank + 8, :] = jnp.broadcast_to(squares, (8, part))
    half_copy.wait_recv()
    first_half = jnp.where(core == 0, pair_recv[0], pair_recv[1])
    second_half = jnp.where(core == 0, pair_recv[1], pair_recv[0])
    wide = aug.shape[1] // 2
    aug[:, wide:] = jnp.where(
        lax.broadcasted_iota(jnp.int32, (rank, wide), 0)
        == lax.broadcasted_iota(jnp.int32, (rank, wide), 1),
        1.0,
        0.0,
    )
    aug[:, :wide] = jnp.zeros((rank, wide), F32)
    aug[0:half, 0:rank] = jnp.square((pair_send[0] + first_half) / orbitals_count)
    aug[half:rank, 0:rank] = jnp.square((pair_send[1] + second_half) / orbitals_count)

    def block_step(j, carry):
        start = pl.multiple_of(j * BLOCK, BLOCK)
        strip = aug[pl.ds(start, BLOCK), :]
        pick = jnp.where(
            lax.broadcasted_iota(jnp.int32, (wide, 128), 0)
            == lax.broadcasted_iota(jnp.int32, (wide, 128), 1) + start,
            1.0,
            0.0,
        )
        lane = lax.broadcasted_iota(jnp.int32, (BLOCK, 128), 1)
        row_at = lax.broadcasted_iota(jnp.int32, (BLOCK, 128), 0)
        square = dot_nn(strip[:, :wide], pick, HIGHEST)
        tile = jnp.where(lane < BLOCK, square, jnp.where(lane == row_at + 64, 1.0, 0.0))
        tile = eliminate_small(tile, BLOCK)
        inverse = tile[:, 64 : 64 + BLOCK]
        solved = dot_nn(inverse, strip, HIGHEST)
        head = solved[:, :wide]
        ahead = lax.broadcasted_iota(jnp.int32, (BLOCK, wide), 1) >= start + BLOCK
        multipliers = jnp.where(ahead, head, 0.0)
        aug[...] = aug[...] - dot_tn(multipliers, solved, HIGHEST)[0:rank]
        aug[pl.ds(start, BLOCK), :] = solved
        return carry

    lax.fori_loop(0, rank // BLOCK, block_step, 0)
    lower_inverse = aug[:, wide:]

    count = rank // steps
    best = [None] * steps
    stores = []
    for p in range(PARTS):
        travel[p].wait_recv()
        both = local[p] + arrived[p]
        scaled = jnp.square(both / orbitals_count)
        columns = scaled[0:rank]
        diagonal = scaled[rank : rank + 1]
        solved = dot_nn(lower_inverse[:, 0:rank], columns, HIGHEST)
        out_v[p] = solved.T
        store = pltpu.make_async_copy(
            out_v.at[p], factor_hbm.at[pl.ds(p * part, part), :], out_sem.at[p]
        )
        store.start()
        stores.append(store)
        for s in range(steps):
            piece = solved[s * count : (s + 1) * count]
            diagonal = diagonal - jnp.sum(piece * piece, axis=0, keepdims=True)
            best[s] = diagonal if best[s] is None else jnp.maximum(best[s], diagonal)
        diag_ref[:, p * part : (p + 1) * part] = diagonal

    row8 = lax.broadcasted_iota(jnp.int32, (8, 128), 0)
    tile = jnp.zeros((8, 128), F32)
    for s in range(steps):
        top = jnp.max(best[s], axis=1, keepdims=True)
        tile = jnp.where(row8 == s, jnp.broadcast_to(top, (8, 128)), tile)
    tile_mine[0] = tile
    round_orb = []
    for d in range(1, n_orb):
        copy = pltpu.make_async_remote_copy(
            src_ref=tile_mine.at[0], dst_ref=tile_orb.at[d],
            send_sem=mo_send.at[d], recv_sem=mo_recv.at[d],
            device_id=(g, lax.rem(o + d, n_orb)), device_id_type=MESH,
        )
        copy.start()
        round_orb.append(copy)
    for d in range(1, n_orb):
        round_orb[d - 1].wait_recv()
        tile = jnp.maximum(tile, tile_orb[d])
    tile_mine[1] = tile
    round_grid = []
    for d in range(1, n_grid):
        copy = pltpu.make_async_remote_copy(
            src_ref=tile_mine.at[1], dst_ref=tile_grid.at[d],
            send_sem=mg_send.at[d], recv_sem=mg_recv.at[d],
            device_id=(lax.rem(g + d, n_grid), o), device_id_type=MESH,
        )
        copy.start()
        round_grid.append(copy)
    for d in range(1, n_grid):
        round_grid[d - 1].wait_recv()
        tile = jnp.maximum(tile, tile_grid[d])
    peaks_ref[...] = tile

    for store in stores:
        store.wait()
    for d in range(1, n_grid):
        target, copy = first(d)

        @pl.when(target < slots)
        def _(copy=copy):
            copy.wait_send()

    @pl.when(g < slots)
    def _():
        for d in range(1, n_grid):
            second(d).wait_send()

    for copy in crossing + [swap_copy, pair_copy, half_copy] + travel + round_orb + round_grid:
        copy.wait_send()


def solution(mesh):
    n_grid, n_orb = mesh.shape["grid"], mesh.shape["orb"]
    assert n_orb == 4

    def on_device(orbitals, pivots):
        depth, rows = orbitals.shape
        steps, count = pivots.shape
        rank = steps * count
        share = rows // n_orb
        part = share // PARTS
        slot_rows = -(-rank // n_grid)
        slot_rows = -(-slot_rows // 16) * 16
        while rank % slot_rows:
            slot_rows += 16
        slots = rank // slot_rows
        wide = -(-rank // 128) * 128
        dma = pltpu.SemaphoreType.DMA
        vmem = pltpu.VMEM
        factor, diagonal, peaks = pl.pallas_call(
            functools.partial(kernel, n_grid, n_orb, steps, depth * n_orb),
            out_shape=(
                jax.ShapeDtypeStruct((share, rank), F32),
                jax.ShapeDtypeStruct((1, share), F32),
                jax.ShapeDtypeStruct((8, 128), F32),
            ),
            in_specs=[
                pl.BlockSpec(memory_space=pl.ANY),
                pl.BlockSpec(memory_space=vmem),
            ],
            out_specs=(
                pl.BlockSpec(memory_space=pl.ANY),
                pl.BlockSpec(memory_space=vmem),
                pl.BlockSpec(memory_space=vmem),
            ),
            scratch_shapes=[
                vmem((n_orb, depth, share), BF16),
                vmem((2, depth, share), BF16),
                vmem((slots, slot_rows, depth), BF16),
                vmem((slots, slot_rows, depth), BF16),
                vmem((n_grid, slot_rows, depth), BF16),
                vmem((slots, slot_rows, depth), BF16),
                vmem((PARTS, rank + 8, part), F32),
                vmem((PARTS, rank + 8, part), F32),
                vmem((PARTS, rank + 8, part), F32),
                vmem((2, rank // 2, rank), F32),
                vmem((2, rank // 2, rank), F32),
                vmem((rank, 2 * wide), F32),
                vmem((PARTS, part, rank), F32),
                vmem((2, 8, 128), F32),
                vmem((n_orb, 8, 128), F32),
                vmem((n_grid, 8, 128), F32),
                dma((n_orb,)), dma((PARTS,)), dma((2,)), dma((2,)),
                dma((n_grid,)), dma((n_grid,)), dma((n_grid,)), dma((n_grid,)),
                dma, dma, dma, dma, dma, dma, dma((PARTS,)), dma((PARTS,)),
                dma((n_orb,)), dma((n_orb,)), dma((n_grid,)), dma((n_grid,)),
            ],
            compiler_params=pltpu.CompilerParams(
                collective_id=0, has_side_effects=True, vmem_limit_bytes=58 * 1024 * 1024
            ),
        )(orbitals, pivots.reshape(rank, 1))
        return factor, diagonal.reshape(share), peaks[:steps, 0]

    return jax.shard_map(
        on_device,
        mesh=mesh,
        in_specs=(P("orb", "grid"), P()),
        out_specs=(P(("grid", "orb"), None), P(("grid", "orb")), P()),
        check_vma=False,
    )
```

```python
import functools

import jax
import jax.numpy as jnp
from jax import lax
from jax.experimental import pallas as pl
from jax.experimental.pallas import tpu as pltpu
from jax.sharding import PartitionSpec as P

F32 = jnp.float32
BF16 = jnp.bfloat16
HIGHEST = lax.Precision.HIGHEST
MESH = pl.DeviceIdType.MESH
BLOCK = 48
PARTS = 4


def dot_nn(a, b, precision=None):
    return lax.dot_general(
        a, b, (((1,), (0,)), ((), ())), precision=precision, preferred_element_type=F32
    )


def dot_nt(a, b, precision=None):
    return lax.dot_general(
        a, b, (((1,), (1,)), ((), ())), precision=precision, preferred_element_type=F32
    )


def dot_tn(a, b, precision=None):
    return lax.dot_general(
        a, b, (((0,), (0,)), ((), ())), precision=precision, preferred_element_type=F32
    )


def eliminate_small(t, size):
    row_at = lax.broadcasted_iota(jnp.int32, t.shape, 0)
    for k in range(size):
        scale = lax.rsqrt(t[k : k + 1, k : k + 1])
        row = t[k : k + 1, :] * scale
        column = t[:, k : k + 1] * scale
        t = jnp.where(row_at > k, t - column * row, jnp.where(row_at == k, row, t))
    return t


def kernel(
    n_grid, n_orb, steps, orbitals_count,
    orb_hbm, piv_ref,
    factor_hbm, diag_ref, peaks_ref,
    own, other, mine, total, heard, swap, sums, arrived, side_sums, side_arrived, local, pair_send, pair_recv,
    aug, out_v, tile_mine, tile_orb, tile_grid,
    load_sem, out_sem, x_send, x_recv, p1_send, p1_recv, p2_send, p2_recv,
    c_send, c_recv, q_send, q_recv, h_send, h_recv, s_send, s_recv, z_send, z_recv,
    mo_send, mo_recv, mg_send, mg_recv,
):
    g = lax.axis_index("grid")
    o = lax.axis_index("orb")
    core = lax.rem(o, 2)
    side = o // 2
    mate = o + 1 - 2 * core
    across = (1 - side) * 2 + core
    share = own.shape[2]
    slots, slot_rows, _ = mine.shape
    rank = slots * slot_rows
    part = share // PARTS
    rows = share * n_orb

    loads = []
    for b in range(n_orb):
        copy = pltpu.make_async_copy(
            orb_hbm.at[:, pl.ds(b * share, share)], own.at[b], load_sem.at[b]
        )
        copy.start()
        loads.append(copy)

    barrier = pltpu.get_barrier_semaphore()
    for d in range(1, n_grid):
        pl.semaphore_signal(
            barrier, inc=1, device_id=(lax.rem(g + d, n_grid), o), device_id_type=MESH
        )
    for d in range(1, n_orb):
        pl.semaphore_signal(
            barrier, inc=1, device_id=(g, lax.rem(o + d, n_orb)), device_id_type=MESH
        )
    pl.semaphore_wait(barrier, n_grid + n_orb - 2)

    crossing = []
    for yy in range(2):
        start = pl.multiple_of((yy * 2 + 1 - core) * share, share)
        copy = pltpu.make_async_remote_copy(
            src_ref=orb_hbm.at[:, pl.ds(start, share)],
            dst_ref=other.at[yy],
            send_sem=x_send.at[yy],
            recv_sem=x_recv.at[yy],
            device_id=(g, mate),
            device_id_type=MESH,
        )
        copy.start()
        crossing.append(copy)

    base = g * rows
    wanted = piv_ref[...] - base
    picked = None
    for b in range(n_orb):
        loads[b].wait()
        lanes = lax.broadcasted_iota(jnp.int32, (rank, share), 1) + b * share
        hot = jnp.where(lanes == wanted, 1.0, 0.0).astype(BF16)
        term = dot_nt(hot, own[b])
        picked = term if picked is None else picked + term
    picked = picked.astype(BF16)
    for s in range(slots):
        mine[s] = picked[s * slot_rows : (s + 1) * slot_rows]

    def first(d):
        target = lax.rem(g + d, n_grid)
        return target, pltpu.make_async_remote_copy(
            src_ref=mine.at[lax.rem(target, slots)],
            dst_ref=heard.at[d],
            send_sem=p1_send.at[d],
            recv_sem=p1_recv.at[d],
            device_id=(target, o),
            device_id_type=MESH,
        )

    def second(d):
        target = lax.rem(g + d, n_grid)
        return pltpu.make_async_remote_copy(
            src_ref=heard.at[0],
            dst_ref=total.at[lax.rem(g, slots)],
            send_sem=p2_send.at[d],
            recv_sem=p2_recv.at[d],
            device_id=(target, o),
            device_id_type=MESH,
        )

    for d in range(1, n_grid):
        target, copy = first(d)

        @pl.when(target < slots)
        def _(copy=copy):
            copy.start()

    @pl.when(g < slots)
    def _():
        added = mine[lax.rem(g, slots)]
        for d in range(1, n_grid):
            first(d)[1].wait_recv()
            added = added + heard[d]
        heard[0] = added
        for d in range(1, n_grid):
            second(d).start()
        total[lax.rem(g, slots)] = added

    for copy in crossing:
        copy.wait_recv()

    def moments(block, yy, p):
        lo = p * part
        a = own[block, :, lo : lo + part]
        b = other[yy, :, lo : lo + part]
        a32 = a.astype(F32)
        b32 = b.astype(F32)
        squares = jnp.sum(a32 * a32, axis=0, keepdims=True) + jnp.sum(
            b32 * b32, axis=0, keepdims=True
        )
        point_sum = jnp.sum(a32, axis=0, keepdims=True) + jnp.sum(b32, axis=0, keepdims=True)
        return squares, point_sum

    for p in range(PARTS):
        squares, point_sum = moments(across, 1 - side, p)
        side_sums[p] = jnp.zeros((8, part), F32)
        side_sums[p, 0:1] = squares
        side_sums[p, 1:2] = point_sum
        squares, _ = moments(o, side, p)
        local[p, rank : rank + 8, :] = jnp.broadcast_to(squares, (8, part))

    for d in range(1, n_grid):
        source = lax.rem(g + n_grid - d, n_grid)

        @pl.when(source < slots)
        def _(d=d):
            second(d).wait_recv()

    swap_copy = pltpu.make_async_remote_copy(
        src_ref=total, dst_ref=swap, send_sem=c_send, recv_sem=c_recv,
        device_id=(g, mate), device_id_type=MESH,
    )
    swap_copy.start()
    here = jnp.reshape(total[...], (rank, total.shape[2]))
    pair_here = dot_nt(here, here)
    swap_copy.wait_recv()
    there = jnp.reshape(swap[...], (rank, swap.shape[2]))
    pair = pair_here + dot_nt(there, there)
    half = rank // 2
    pivot_mean = (
        jnp.sum(here.astype(F32), axis=1, keepdims=True)
        + jnp.sum(there.astype(F32), axis=1, keepdims=True)
    ) / (2.0 * total.shape[2])
    for h in range(2):
        pair_send[h, :, 0:rank] = pair[h * half : (h + 1) * half]
        pair_send[h, :, rank : rank + 1] = pivot_mean[h * half : (h + 1) * half]
    pair_copy = pltpu.make_async_remote_copy(
        src_ref=pair_send.at[core], dst_ref=pair_recv.at[0], send_sem=q_send, recv_sem=q_recv,
        device_id=(g, across), device_id_type=MESH,
    )
    pair_copy.start()

    def products(block, yy, p):
        lo = p * part
        a = own[block, :, lo : lo + part]
        b = other[yy, :, lo : lo + part]
        return dot_nn(here, a) + dot_nn(there, b)


    travel = []
    for p in range(PARTS):
        inner = products(across, 1 - side, p)
        squares = side_sums[p, 0:1]
        point_sum = side_sums[p, 1:2]
        rest = inner - pivot_mean * point_sum
        most = jnp.max(jnp.abs(rest), axis=0, keepdims=True)
        step = jnp.maximum(most * (1.0 / 32767.0), 1e-30)
        coded = jnp.round(rest * (1.0 / step))
        sums[p] = jnp.clip(coded, -32767.0, 32767.0).astype(jnp.int32).astype(jnp.int16)
        side_sums[p, 2:3] = step
        for copy in (
            pltpu.make_async_remote_copy(
                src_ref=side_sums.at[p], dst_ref=side_arrived.at[p],
                send_sem=z_send.at[p], recv_sem=z_recv.at[p],
                device_id=(g, across), device_id_type=MESH,
            ),
            pltpu.make_async_remote_copy(
                src_ref=sums.at[p], dst_ref=arrived.at[p],
                send_sem=s_send.at[p], recv_sem=s_recv.at[p],
                device_id=(g, across), device_id_type=MESH,
            ),
        ):
            copy.start()
            travel.append(copy)

    pair_copy.wait_recv()
    half_copy = pltpu.make_async_remote_copy(
        src_ref=pair_recv.at[0], dst_ref=pair_recv.at[1], send_sem=h_send, recv_sem=h_recv,
        device_id=(g, mate), device_id_type=MESH,
    )
    half_copy.start()
    for p in range(PARTS):
        local[p, 0:rank, :] = products(o, side, p)
    half_copy.wait_recv()
    first_half = jnp.where(core == 0, pair_recv[0], pair_recv[1])
    second_half = jnp.where(core == 0, pair_recv[1], pair_recv[0])
    wide = aug.shape[1]
    aug[...] = jnp.zeros((rank, wide), F32)
    aug[0:half, 0:rank] = jnp.square((pair_send[0] + first_half)[:, 0:rank] / orbitals_count)
    aug[half:rank, 0:rank] = jnp.square((pair_send[1] + second_half)[:, 0:rank] / orbitals_count)
    far_mean = jnp.concatenate(
        [first_half[:, rank : rank + 1], second_half[:, rank : rank + 1]], axis=0
    )

    def block_step(j, carry):
        start = pl.multiple_of(j * BLOCK, BLOCK)
        strip = aug[pl.ds(start, BLOCK), :]
        pick = jnp.where(
            lax.broadcasted_iota(jnp.int32, (wide, 128), 0)
            == lax.broadcasted_iota(jnp.int32, (wide, 128), 1) + start,
            1.0,
            0.0,
        )
        lane = lax.broadcasted_iota(jnp.int32, (BLOCK, 128), 1)
        row_at = lax.broadcasted_iota(jnp.int32, (BLOCK, 128), 0)
        square = dot_nn(strip, pick, HIGHEST)
        tile = jnp.where(lane < BLOCK, square, jnp.where(lane == row_at + 64, 1.0, 0.0))
        tile = eliminate_small(tile, BLOCK)
        inverse = tile[:, 64 : 64 + BLOCK]
        at = lax.broadcasted_iota(jnp.int32, (BLOCK, wide), 1)
        unit = jnp.where(at == lax.broadcasted_iota(jnp.int32, (BLOCK, wide), 0) + start, 1.0, 0.0)
        solved = dot_nn(
            inverse, jnp.where((at >= start) & (at < start + BLOCK), unit, strip), HIGHEST
        )
        multipliers = jnp.where(at >= start + BLOCK, solved, 0.0)
        every_lane = lax.broadcasted_iota(jnp.int32, (rank, wide), 1)
        every_row = lax.broadcasted_iota(jnp.int32, (rank, wide), 0)
        clear = (
            (every_lane >= start) & (every_lane < start + BLOCK) & (every_row >= start + BLOCK)
        )
        aug[...] = jnp.where(clear, 0.0, aug[...]) - dot_tn(multipliers, solved, HIGHEST)[0:rank]
        aug[pl.ds(start, BLOCK), :] = jnp.where(at < start + BLOCK, solved, 0.0)
        return carry

    lax.fori_loop(0, rank // BLOCK, block_step, 0)
    lower_inverse = aug[...]

    count = rank // steps
    best = [None] * steps
    stores = []
    for p in range(PARTS):
        travel[2 * p].wait_recv()
        travel[2 * p + 1].wait_recv()
        far = side_arrived[p]
        inner = (
            local[p, 0:rank, :]
            + arrived[p].astype(jnp.int32).astype(F32) * far[2:3]
            + far_mean * far[1:2]
        )
        columns = jnp.square(inner / orbitals_count)
        diagonal = jnp.square((local[p, rank : rank + 1, :] + far[0:1]) / orbitals_count)
        solved = dot_nn(lower_inverse[:, 0:rank], columns, HIGHEST)
        out_v[p] = solved.T
        store = pltpu.make_async_copy(
            out_v.at[p], factor_hbm.at[pl.ds(p * part, part), :], out_sem.at[p]
        )
        store.start()
        stores.append(store)
        for s in range(steps):
            piece = solved[s * count : (s + 1) * count]
            diagonal = diagonal - jnp.sum(piece * piece, axis=0, keepdims=True)
            best[s] = diagonal if best[s] is None else jnp.maximum(best[s], diagonal)
        diag_ref[:, p * part : (p + 1) * part] = diagonal

    row8 = lax.broadcasted_iota(jnp.int32, (8, 128), 0)
    tile = jnp.zeros((8, 128), F32)
    for s in range(steps):
        top = jnp.max(best[s], axis=1, keepdims=True)
        tile = jnp.where(row8 == s, jnp.broadcast_to(top, (8, 128)), tile)
    tile_mine[0] = tile
    round_orb = []
    for d in range(1, n_orb):
        copy = pltpu.make_async_remote_copy(
            src_ref=tile_mine.at[0], dst_ref=tile_orb.at[d],
            send_sem=mo_send.at[d], recv_sem=mo_recv.at[d],
            device_id=(g, lax.rem(o + d, n_orb)), device_id_type=MESH,
        )
        copy.start()
        round_orb.append(copy)
    for d in range(1, n_orb):
        round_orb[d - 1].wait_recv()
        tile = jnp.maximum(tile, tile_orb[d])
    tile_mine[1] = tile
    round_grid = []
    for d in range(1, n_grid):
        copy = pltpu.make_async_remote_copy(
            src_ref=tile_mine.at[1], dst_ref=tile_grid.at[d],
            send_sem=mg_send.at[d], recv_sem=mg_recv.at[d],
            device_id=(lax.rem(g + d, n_grid), o), device_id_type=MESH,
        )
        copy.start()
        round_grid.append(copy)
    for d in range(1, n_grid):
        round_grid[d - 1].wait_recv()
        tile = jnp.maximum(tile, tile_grid[d])
    peaks_ref[...] = tile

    for store in stores:
        store.wait()
    for d in range(1, n_grid):
        target, copy = first(d)

        @pl.when(target < slots)
        def _(copy=copy):
            copy.wait_send()

    @pl.when(g < slots)
    def _():
        for d in range(1, n_grid):
            second(d).wait_send()

    for copy in crossing + [swap_copy, pair_copy, half_copy] + travel + round_orb + round_grid:
        copy.wait_send()


def solution(mesh):
    n_grid, n_orb = mesh.shape["grid"], mesh.shape["orb"]
    assert n_orb == 4

    def on_device(orbitals, pivots):
        depth, rows = orbitals.shape
        steps, count = pivots.shape
        rank = steps * count
        share = rows // n_orb
        part = share // PARTS
        slot_rows = -(-rank // n_grid)
        slot_rows = -(-slot_rows // 16) * 16
        while rank % slot_rows:
            slot_rows += 16
        slots = rank // slot_rows
        wide = -(-rank // 128) * 128
        dma = pltpu.SemaphoreType.DMA
        vmem = pltpu.VMEM
        factor, diagonal, peaks = pl.pallas_call(
            functools.partial(kernel, n_grid, n_orb, steps, depth * n_orb),
            out_shape=(
                jax.ShapeDtypeStruct((share, rank), F32),
                jax.ShapeDtypeStruct((1, share), F32),
                jax.ShapeDtypeStruct((8, 128), F32),
            ),
            in_specs=[
                pl.BlockSpec(memory_space=pl.ANY),
                pl.BlockSpec(memory_space=vmem),
            ],
            out_specs=(
                pl.BlockSpec(memory_space=pl.ANY),
                pl.BlockSpec(memory_space=vmem),
                pl.BlockSpec(memory_space=vmem),
            ),
            scratch_shapes=[
                vmem((n_orb, depth, share), BF16),
                vmem((2, depth, share), BF16),
                vmem((slots, slot_rows, depth), BF16),
                vmem((slots, slot_rows, depth), BF16),
                vmem((n_grid, slot_rows, depth), BF16),
                vmem((slots, slot_rows, depth), BF16),
                vmem((PARTS, rank, part), jnp.int16),
                vmem((PARTS, rank, part), jnp.int16),
                vmem((PARTS, 8, part), F32),
                vmem((PARTS, 8, part), F32),
                vmem((PARTS, rank + 8, part), F32),
                vmem((2, rank // 2, rank + 1), F32),
                vmem((2, rank // 2, rank + 1), F32),
                vmem((rank, wide), F32),
                vmem((PARTS, part, rank), F32),
                vmem((2, 8, 128), F32),
                vmem((n_orb, 8, 128), F32),
                vmem((n_grid, 8, 128), F32),
                dma((n_orb,)), dma((PARTS,)), dma((2,)), dma((2,)),
                dma((n_grid,)), dma((n_grid,)), dma((n_grid,)), dma((n_grid,)),
                dma, dma, dma, dma, dma, dma, dma((PARTS,)), dma((PARTS,)),
                dma((PARTS,)), dma((PARTS,)),
                dma((n_orb,)), dma((n_orb,)), dma((n_grid,)), dma((n_grid,)),
            ],
            compiler_params=pltpu.CompilerParams(
                collective_id=0, has_side_effects=True, vmem_limit_bytes=58 * 1024 * 1024
            ),
        )(orbitals, pivots.reshape(rank, 1))
        return factor, diagonal.reshape(share), peaks[:steps, 0]

    return jax.shard_map(
        on_device,
        mesh=mesh,
        in_specs=(P("orb", "grid"), P()),
        out_specs=(P(("grid", "orb"), None), P(("grid", "orb")), P()),
        check_vma=False,
    )
```
